32 devices in a mesh: row: 8 (over y, x, core), col: 4 (over z).
Axes of the slice: x: 2, y: 2, z: 4, core: 2. Of those that a mesh axis runs over, the one named last changes fastest.
Arguments:
- window_rows: bfloat16 [1024, 65536], P('row', 'col'), may hold values from -6 to 6
- omega_cols: bfloat16 [512, 1024], P(None, 'row'), may hold values from -0.1875 to 0.1875
- psi_rows: bfloat16 [65536, 1024], P(('col', 'row')), may hold values from -0.046875 to 0.046875
- upsilon_rows: bfloat16 [65536, 2048], P(('col', 'row')), may hold values from -0.046875 to 0.046875
- phi_cols: bfloat16 [2048, 1024], P(None, 'row'), may hold values from -0.1875 to 0.1875
- range_old: float32 [512, 65536], P(None, ('col', 'row')), may hold values from -6 to 6
- core_old: float32 [2048, 2048], P('row', 'col'), may hold values from -6 to 6
Outputs:
- range_sketch: float32 [512, 65536], P(None, ('col', 'row'))
- corange_sketch: float32 [1024, 1024], P('row', 'col')
- core_sketch: float32 [2048, 2048], P('row', 'col')
The draws below stay inside these ranges and needn't reach their ends.
All inputs are finite; a program needn't handle non-finite values.
Results may differ from the reference program's by a relative error of at most 0.0022.
Values may be sent and summed in bfloat16 or wider, within the bound.
A program may use at most 128 MiB of HBM per device.

```python
import jax
import jax.numpy as jnp

NCOLS = 65536
K = 512
L = 1024
S = 2048
WINDOW = 1024


def with_spikes(result, own_key, source, target, blocks, factor):
    def block_of(axis_at):
        return (jnp.arange(result.shape[axis_at]) // (result.shape[axis_at] // blocks)).reshape((-1,) + (1,) * (result.ndim - 1 - axis_at))

    first = jax.random.permutation(own_key, blocks)[block_of(target)]
    far = (block_of(target) + blocks // 2) % blocks
    return jnp.where((block_of(source) == first) | (block_of(source) == far), factor * result, result)


def block_levels(rng, shape, split, least, largest):
    factor_of = 1.0
    for position, parts in split:
        heights = jax.random.uniform(jax.random.fold_in(jax.random.fold_in(rng, 6), position), (parts,), jnp.float32, least / len(split), largest / len(split))
        factor_of = factor_of * jnp.repeat(jnp.exp(heights), shape[position] // parts).reshape((-1,) + (1,) * (len(shape) - 1 - position))
    return factor_of


def gaussian(own_key, extent, deviation, most, shards=(), kind=jnp.bfloat16):
    result = deviation * jax.random.normal(own_key, extent, jnp.float32)
    if shards:
        result = result * block_levels(own_key, extent, shards, -0.22, 0.18)
    return jnp.clip(result, -most, most).astype(kind)


def bell_draw_with(key, dims, deviation, bound, pieces, heavy, dtype=jnp.bfloat16):
    result = deviation * jax.random.normal(key, dims, jnp.float32)
    if pieces:
        result = result * block_levels(key, dims, pieces, -0.22, 0.18)
    return jnp.clip(with_spikes(result, jax.random.fold_in(key, 3), *heavy), -bound, bound).astype(dtype)


def setup_inputs(seed: int = 0) -> dict:
    key_list = jax.random.split(jax.random.key(seed), 8)
    return {
        "window_rows": gaussian(key_list[0], (WINDOW, NCOLS), 1.0, 6.0, ((0, 8), (1, 4))),
        "omega_cols": gaussian(key_list[1], (K, WINDOW), WINDOW ** -0.5, 0.1875, ((1, 8),)),
        "psi_rows": bell_draw_with(key_list[2], (NCOLS, L), NCOLS ** -0.5, 0.046875, ((0, 32),), (0, 1, 32, 2.75)),
        "upsilon_rows": bell_draw_with(key_list[3], (NCOLS, S), NCOLS ** -0.5, 0.046875, ((0, 32),), (0, 1, 32, 2.75)),
        "phi_cols": gaussian(key_list[4], (S, WINDOW), WINDOW ** -0.5, 0.1875, ((1, 8),)),
        "range_old": gaussian(key_list[5], (K, NCOLS), 1.0, 6.0, ((1, 32),), jnp.float32),
        "core_old": gaussian(key_list[6], (S, S), 1.0, 6.0, ((0, 8), (1, 4)), jnp.float32),
    }


def reference(window_rows, omega_cols, psi_rows, upsilon_rows, phi_cols, range_old, core_old):
    range_sketch = range_old + jnp.dot(omega_cols, window_rows, preferred_element_type=jnp.float32)
    corange_sketch = jnp.dot(window_rows, psi_rows, preferred_element_type=jnp.float32)
    sketched = jnp.dot(window_rows, upsilon_rows, preferred_element_type=jnp.float32).astype(jnp.bfloat16)
    core_sketch = core_old + jnp.dot(phi_cols, sketched, preferred_element_type=jnp.float32)
    return range_sketch, corange_sketch, core_sketch
```

```python
import functools

import jax
import jax.numpy as jnp
from jax import lax
from jax.experimental import pallas as pl
from jax.experimental.pallas import tpu as pltpu
from jax.sharding import PartitionSpec as P

MESH = pl.DeviceIdType.MESH
LIMIT = 63 * 1024 * 1024
F32, BF16 = jnp.float32, jnp.bfloat16


def encode(x):
    return (x * jnp.abs(x)).astype(BF16)


def decode(y):
    y = y.astype(F32)
    return y * lax.rsqrt(jnp.maximum(jnp.abs(y), 1e-37))


def flip(index, mask, count):
    total, bit = 0, 1
    while bit < count:
        own = (index // bit) % 2
        total = total + (1 - own if mask & bit else own) * bit
        bit *= 2
    return total


def piece_order(chips):
    classes = {}
    for o in range(chips):
        classes.setdefault(bin(o).count("1"), []).append(o)
    return [(o, h) for k in sorted(classes) for h in range(2) for o in classes[k]]


def sketch_kernel(n, m, window, omega, psi, ups, phi, range_old, core_old, range_out, co_out, core_out,
                  relaid, psi_v, ups_v, xs, xr, keep, zs, z1r, z2r, own, ys, yr, gathered, phi_all, omega_all, range_v,
                  w_sem, l_sem, a_s, a_r, p_s, p_r, x_s, x_r, z_s, z1_s, z2_s, y_s, y_r, g_s, g_r, f_s, f_r, r_sem):
    me, c = lax.axis_index("row"), lax.axis_index("col")
    chips = n // 2
    rows, width = window.shape[0], relaid.shape[1]
    half = rows // 2
    lz = psi_v.shape[1] // m
    sz = ups_v.shape[1] // m
    cz = lz + sz
    slots = keep.shape[0]
    core_rows, depth = phi_all.shape[0], phi.shape[1]
    pieces = piece_order(chips)
    odd = c % 2
    side = c + odd * (m - 1 - 2 * c)
    first = m - 1 - side
    near = c + 1 - 2 * odd
    pair = c // 2

    def at(r, h):
        return pl.ds(pl.multiple_of(r * rows + h * half, half), half)

    def block(r, size):
        return pl.ds(pl.multiple_of(r * size, size), size)

    def peer(mask):
        return flip(me, mask, n)

    def chunk(t):
        ahead = jnp.where(t < first, m - 1 - t, jnp.where(t < m - 1, t - first, side))
        return ahead + odd * (m - 1 - 2 * ahead)

    def remote(src, dst, send_sem, recv_sem, device):
        return pltpu.make_async_remote_copy(
            src_ref=src, dst_ref=dst, send_sem=send_sem, recv_sem=recv_sem, device_id=device, device_id_type=MESH)

    def weights(d):
        return (
            pltpu.make_async_copy(psi.at[:, block(d, lz)], psi_v.at[:, block(d, lz)], w_sem.at[d, 0]),
            pltpu.make_async_copy(ups.at[:, block(d, sz)], ups_v.at[:, block(d, sz)], w_sem.at[d, 1]))

    local = [
        pltpu.make_async_copy(window.at[pl.ds(h * half, half), block(me, width)], relaid.at[at(me, h), :], l_sem.at[h])
        for h in range(2)]
    local += [
        pltpu.make_async_copy(phi.at[block(me, core_rows), :], phi_all.at[:, block(me, depth)], l_sem.at[2]),
        pltpu.make_async_copy(omega, omega_all.at[:, block(me, depth)], l_sem.at[3]),
        pltpu.make_async_copy(range_old, range_v, l_sem.at[4]),
        pltpu.make_async_copy(core_old, core_out, l_sem.at[5])]

    for copy in local[:2]:
        copy.start()
    for t in range(m):
        for copy in weights(chunk(t)):
            copy.start()

    barrier = pltpu.get_barrier_semaphore()
    for e in range(1, n):
        pl.semaphore_signal(barrier, inc=1, device_id={"row": peer(e)}, device_id_type=MESH)
    for d in range(1, m):
        pl.semaphore_signal(barrier, inc=1, device_id={"col": lax.rem(c + d, m)}, device_id_type=MESH)
    pl.semaphore_wait(barrier, n - 1 + m - 1)

    def window_copy(e, h):
        return remote(window.at[pl.ds(h * half, half), block(peer(e), width)], relaid.at[at(me, h), :],
                      a_s.at[e, h], a_r.at[e, h], {"row": peer(e)})

    def phi_copy(e):
        return remote(phi.at[block(peer(e), core_rows), :], phi_all.at[:, block(me, depth)],
                      p_s.at[e], p_r.at[e], {"row": peer(e)})

    for o, h in pieces:
        for e in (2 * o, 2 * o + 1):
            if e:
                window_copy(e, h).start()

    def spread_omega(o):
        return remote(omega, omega_all.at[:, block(me, depth)], g_s.at[o, 2], g_r.at[o, 2], {"row": peer(2 * o)})

    def pass_omega(o):
        place = omega_all.at[:, block(peer(2 * o), depth)]
        return remote(place, place, f_s.at[o, 2], f_r.at[o, 2], {"row": peer(1)})

    def spread_rows(o, h):
        place = gathered.at[at(me, h), :]
        return remote(place, place, g_s.at[o, h], g_r.at[o, h], {"row": peer(2 * o)})

    def pass_rows(o, h):
        place = gathered.at[at(peer(2 * o), h), :]
        return remote(place, place, f_s.at[o, h], f_r.at[o, h], {"row": peer(1)})

    for copy in local[2:]:
        copy.start()
    for e in range(1, n):
        phi_copy(e).start()
    for o in range(1, chips):
        spread_omega(o).start()
    local[3].wait()
    pass_omega(0).start()

    def swap_copy(i, d):
        return remote(xs.at[i % slots, d], xr.at[i, d], x_s.at[i, d], x_r.at[i, d], {"row": peer(1)})

    def near_copy(i, d):
        return remote(zs.at[i, d], z1r.at[i, d], z_s.at[i, d], z1_s.at[i, d], {"col": near})

    def far_copy(i, d):
        return remote(zs.at[i, d], z2r.at[i, pair], z_s.at[i, d], z2_s.at[i, pair], {"col": d})

    def back_copy(i):
        o, h = pieces[i]
        return remote(ys.at[i], yr.at[o, h], y_s.at[i], y_r.at[o, h], {"row": peer(2 * o)})

    def multiply(i):
        o, h = pieces[i]
        slot = i % slots
        if o == 0:
            local[h].wait()
        else:
            window_copy(2 * o, h).wait_recv()
        window_copy(2 * o + 1, h).wait_recv()

        @pl.loop(0, m)
        def _(t):
            d = chunk(t)
            if i == 0:
                for copy in weights(d):
                    copy.wait()
            if i >= slots:
                swap_copy(i - slots, d).wait_send()
            lhs = jnp.concatenate([relaid[at(peer(2 * o + 1), h), :], relaid[at(peer(2 * o), h), :]], axis=0)
            for weight, w, start in ((psi_v, lz, 0), (ups_v, sz, lz)):
                product = jnp.dot(lhs, weight[:, block(d, w)], preferred_element_type=F32)
                xs[slot, d, :, start:start + w] = product[:half]
                keep[slot, d, :, start:start + w] = product[half:]
            swap_copy(i, d).start()

    def combine(i):
        slot = i % slots

        @pl.loop(0, m)
        def _(t):
            d = chunk(t)
            swap_copy(i, d).wait_recv()
            total = keep[slot, d] + xr[i, d]

            @pl.when(t < first)
            def _():
                zs[i, d] = encode(total)
                near_copy(i, d).start()

            @pl.when(t >= first)
            def _():
                keep[slot, d] = total

    def relay(i):
        slot = i % slots

        @pl.loop(first, m - 1)
        def _(t):
            d = chunk(t)
            near_copy(i, d).wait_recv()
            zs[i, d] = encode(keep[slot, d] + decode(z1r[i, d]))
            far_copy(i, d).start()

    def give_back(i):
        o, h = pieces[i]
        near_copy(i, c).wait_recv()
        own_slot = own.at[h] if o == 0 else keep.at[i % slots, c]
        own_slot[...] = keep[i % slots, c] + decode(z1r[i, c])
        for g in range(m // 2):
            @pl.when(g != pair)
            def _():
                remote(zs.at[i, c], z2r.at[i, g], z_s.at[i, c], z2_s.at[i, g], {"col": near}).wait_recv()
                own_slot[...] += decode(z2r[i, g])
        if o:
            ys[i] = encode(own_slot[...])
            back_copy(i).start()

    def finish(h):
        total = own[h]
        for o in range(1, chips):
            back_copy(pieces.index((o, h))).wait_recv()
            total = total + decode(yr[o, h])
        co_out[pl.ds(h * half, half), :] = total[:, :lz]
        gathered[at(me, h), :] = total[:, lz:].astype(BF16)
        for o in range(1, chips):
            spread_rows(o, h).start()
        pass_rows(0, h).start()

    count = len(pieces)
    for step in range(count + 2):
        if step < count:
            multiply(step)
            combine(step)
        if 0 <= step - 1 < count:
            relay(step - 1)
        if 0 <= step - 2:
            give_back(step - 2)

    for h in range(2):
        finish(h)

    for o in range(1, chips):
        spread_omega(o).wait_recv()
        pass_omega(o).start()
    for h in range(2):
        for o in range(1, chips):
            spread_rows(o, h).wait_recv()
            pass_rows(o, h).start()
    for o in range(chips):
        pass_omega(o).wait_recv()
    local[4].wait()
    tile = range_tile(width)

    def range_copy(j):
        return pltpu.make_async_copy(range_v.at[:, block(j, tile)], range_out.at[:, block(j, tile)], r_sem.at[j])

    @pl.loop(0, width // tile)
    def _(j):
        range_v[:, block(j, tile)] += jnp.dot(omega_all[...], relaid[:, block(j, tile)], preferred_element_type=F32)
        range_copy(j).start()

    local[2].wait()
    local[5].wait()
    for e in range(1, n):
        phi_copy(e).wait_recv()
    for h in range(2):
        for o in range(chips):
            pass_rows(o, h).wait_recv()
    core_out[...] += jnp.dot(phi_all[...], gathered[...], preferred_element_type=F32)

    for e in range(1, n):
        phi_copy(e).wait_send()
        for h in range(2):
            window_copy(e, h).wait_send()
    for o in range(chips):
        pass_omega(o).wait_send()
        if o:
            spread_omega(o).wait_send()
        for h in range(2):
            pass_rows(o, h).wait_send()
            if o:
                spread_rows(o, h).wait_send()
    for i in range(count):
        if pieces[i][0]:
            back_copy(i).wait_send()

        @pl.loop(0, m)
        def _(d):
            if i + slots >= count:
                swap_copy(i, d).wait_send()

            @pl.when(d != c)
            def _():
                near_copy(i, d).wait_send()

    @pl.loop(0, width // tile)
    def _(j):
        range_copy(j).wait()


def range_tile(width):
    return min(width, 256)


def shards(n, m, window_rows, omega_cols, psi_rows, upsilon_rows, phi_cols, range_old, core_old):
    any_space = pl.BlockSpec(memory_space=pl.ANY)
    vmem = pl.BlockSpec(memory_space=pltpu.VMEM)
    dma = pltpu.SemaphoreType.DMA
    rows, wide = window_rows.shape
    width = wide // n
    k = omega_cols.shape[0]
    l, s = psi_rows.shape[1], upsilon_rows.shape[1]
    core_rows = phi_cols.shape[0] // n
    half, chips, cz = rows // 2, n // 2, (l + s) // m
    count = 2 * chips
    slots = min(count, 4)
    scratch = [
        pltpu.VMEM((rows * n, width), BF16), pltpu.VMEM((width, l), BF16), pltpu.VMEM((width, s), BF16),
        pltpu.VMEM((slots, m, half, cz), F32), pltpu.VMEM((count, m, half, cz), F32), pltpu.VMEM((slots, m, half, cz), F32),
        pltpu.VMEM((count, m, half, cz), BF16), pltpu.VMEM((count, m, half, cz), BF16), pltpu.VMEM((count, m // 2, half, cz), BF16),
        pltpu.VMEM((2, half, cz), F32), pltpu.VMEM((count, half, cz), BF16), pltpu.VMEM((chips, 2, half, cz), BF16),
        pltpu.VMEM((rows * n, s // m), BF16), pltpu.VMEM((core_rows, rows * n), BF16), pltpu.VMEM((k, rows * n), BF16),
        pltpu.VMEM((k, width), F32),
        dma((m, 2)), dma((6,)), dma((n, 2)), dma((n, 2)), dma((n,)), dma((n,)),
        dma((count, m)), dma((count, m)), dma((count, m)), dma((count, m)), dma((count, m // 2)),
        dma((count,)), dma((chips, 2)), dma((chips, 3)), dma((chips, 3)), dma((chips, 3)), dma((chips, 3)),
        dma((width // range_tile(width),)),
    ]
    return pl.pallas_call(
        functools.partial(sketch_kernel, n, m),
        out_shape=(
            jax.ShapeDtypeStruct((k, width), F32), jax.ShapeDtypeStruct((rows, l // m), F32),
            jax.ShapeDtypeStruct((core_rows, s // m), F32)),
        in_specs=[any_space] * 7,
        out_specs=(any_space, vmem, vmem),
        scratch_shapes=scratch,
        compiler_params=pltpu.CompilerParams(collective_id=0, has_side_effects=True, vmem_limit_bytes=LIMIT),
        name="sketch",
    )(window_rows, omega_cols, psi_rows, upsilon_rows, phi_cols, range_old, core_old)


def solution(mesh):
    placed = (
        P("row", "col"),
        P(None, "row"),
        P(("col", "row"), None),
        P(("col", "row"), None),
        P(None, "row"),
        P(None, ("col", "row")),
        P("row", "col"),
    )
    return jax.shard_map(
        functools.partial(shards, mesh.shape["row"], mesh.shape["col"]),
        mesh=mesh,
        in_specs=placed,
        out_specs=(P(None, ("col", "row")), P("row", "col"), P("row", "col")),
        check_vma=False,
    )
```

```python
import contextlib
import functools
import math

import jax
import jax.numpy as jnp
from jax import lax
from jax.experimental import pallas as pl
from jax.experimental.pallas import tpu as pltpu
from jax.sharding import PartitionSpec as P

MESH = pl.DeviceIdType.MESH
LIMIT = 67043328
LEAD = 3
LAG = 2
ROOM = 13000 * 1024
F32, BF16 = jnp.float32, jnp.bfloat16


def mark(name):
    return contextlib.nullcontext()


def encode(x):
    return (x * jnp.abs(x)).astype(BF16)


def decode(y):
    y = y.astype(F32)
    return y * lax.rsqrt(jnp.maximum(jnp.abs(y), 1e-37))


def flip(index, mask, count):
    total, bit = 0, 1
    while bit < count:
        own = (index // bit) % 2
        total = total + (1 - own if mask & bit else own) * bit
        bit *= 2
    return total


def piece_order(chips):
    classes = {}
    for o in range(chips):
        classes.setdefault(bin(o).count("1"), []).append(o)
    return [(o, h) for k in sorted(classes) for h in range(2) for o in classes[k]]


def sketch_kernel(n, m, window, omega, psi, ups, phi, range_old, core_old, range_v, co_out, core_out,
                  relaid, psi_v, ups_v, xs, xr, keep, zs, z1r, z2r, own, ys, yr, gathered, phi_all, omega_all,
                  w_sem, l_sem, a_s, a_r, p_s, p_r, x_s, x_r, z_s, z1_s, z2_s, y_s, y_r, g_s, g_r, f_s, f_r):
    me, c = lax.axis_index("row"), lax.axis_index("col")
    chips = n // 2
    rows, width = window.shape[0], relaid.shape[1]
    half = rows // 2
    lz = psi_v.shape[1] // m
    sz = ups_v.shape[1] // m
    cz = lz + sz
    slots = keep.shape[0]
    core_rows, depth = phi_all.shape[0], phi.shape[1]
    pieces = piece_order(chips)
    odd = c % 2
    side = c + odd * (m - 1 - 2 * c)
    first = m - 1 - side
    near = c + 1 - 2 * odd
    pair = c // 2

    def at(r, h):
        return pl.ds(pl.multiple_of(r * rows + h * half, half), half)

    def block(r, size):
        return pl.ds(pl.multiple_of(r * size, size), size)

    def peer(mask):
        return flip(me, mask, n)

    def chunk(t):
        ahead = jnp.where(t < first, m - 1 - t, jnp.where(t < m - 1, t - first, side))
        return ahead + odd * (m - 1 - 2 * ahead)

    def remote(src, dst, send_sem, recv_sem, device):
        return pltpu.make_async_remote_copy(
            src_ref=src, dst_ref=dst, send_sem=send_sem, recv_sem=recv_sem, device_id=device, device_id_type=MESH)

    def sent(ref, sem):
        remote(ref, ref, sem, y_r.at[0], {"row": peer(1)}).wait_send()

    def received(ref, sem):
        remote(ref, ref, y_s, sem, {"row": peer(1)}).wait_recv()

    def weights(d):
        return (
            pltpu.make_async_copy(psi.at[:, block(d, lz)], psi_v.at[:, block(d, lz)], w_sem.at[d, 0]),
            pltpu.make_async_copy(ups.at[:, block(d, sz)], ups_v.at[:, block(d, sz)], w_sem.at[d, 1]))

    local = [
        pltpu.make_async_copy(window.at[pl.ds(h * half, half), block(me, width)], relaid.at[at(me, h), :], l_sem.at[h])
        for h in range(2)]
    local += [
        pltpu.make_async_copy(phi.at[block(me, core_rows), :], phi_all.at[:, block(me, depth)], l_sem.at[2]),
        pltpu.make_async_copy(omega, omega_all.at[:, block(me, depth)], l_sem.at[3]),
        pltpu.make_async_copy(range_old, range_v, l_sem.at[4]),
        pltpu.make_async_copy(core_old, core_out, l_sem.at[5])]

    for copy in local[:2]:
        copy.start()
    for t in range(m):
        for copy in weights(chunk(t)):
            copy.start()

    barrier = pltpu.get_barrier_semaphore()
    for e in range(1, n):
        pl.semaphore_signal(barrier, inc=1, device_id={"row": peer(e)}, device_id_type=MESH)
    for d in range(1, m):
        pl.semaphore_signal(barrier, inc=1, device_id={"col": lax.rem(c + d, m)}, device_id_type=MESH)
    pl.semaphore_wait(barrier, n - 1 + m - 1)

    def window_copy(e, h):
        return remote(window.at[pl.ds(h * half, half), block(peer(e), width)], relaid.at[at(me, h), :],
                      a_s, a_r.at[e, h], {"row": peer(e)})

    def phi_copy(e):
        return remote(phi.at[block(peer(e), core_rows), :], phi_all.at[:, block(me, depth)],
                      p_s, p_r, {"row": peer(e)})

    def send_window(i):
        o, h = pieces[i]
        for e in (2 * o, 2 * o + 1):
            if e:
                window_copy(e, h).start()

    def distant(i):
        return bin(pieces[i][0]).count("1") > 1

    for i in range(len(pieces)):
        if not distant(i):
            send_window(i)

    def spread_omega(o):
        return remote(omega, omega_all.at[:, block(me, depth)], g_s.at[1], g_r.at[2], {"row": peer(2 * o)})

    def pass_omega(o):
        place = omega_all.at[:, block(peer(2 * o), depth)]
        return remote(place, place, f_s.at[1], f_r.at[2], {"row": peer(1)})

    def spread_rows(o, h):
        place = gathered.at[at(me, h), :]
        return remote(place, place, g_s.at[0], g_r.at[h], {"row": peer(2 * o)})

    def pass_rows(o, h):
        place = gathered.at[at(peer(2 * o), h), :]
        return remote(place, place, f_s.at[0], f_r.at[h], {"row": peer(1)})

    for copy in local[2:]:
        copy.start()

    def send_small():
        for o in range(1, chips):
            spread_omega(o).start()
        local[3].wait()
        pass_omega(0).start()
        for e in range(1, n):
            phi_copy(e).start()

    def swap_copy(i, d):
        return remote(xs.at[i % slots, d], xr.at[i, d], x_s.at[i % slots], x_r.at[i % 2, d], {"row": peer(1)})

    def near_copy(i, d):
        return remote(zs.at[i, d], z1r.at[i, d], z_s, z1_s.at[i, d], {"col": near})

    def far_copy(i, d):
        return remote(zs.at[i, d], z2r.at[i, pair], z_s, z2_s.at[i, pair], {"col": d})

    def back_copy(i):
        o, h = pieces[i]
        return remote(ys.at[i], yr.at[h, o], y_s, y_r.at[h], {"row": peer(2 * o)})

    def multiply(i):
        o, h = pieces[i]
        slot = i % slots
        if o == 0:
            local[h].wait()
        else:
            window_copy(2 * o, h).wait_recv()
        window_copy(2 * o + 1, h).wait_recv()
        if i >= slots:
            sent(xs.at[slot], x_s.at[slot])

        def product(t):
            d = chunk(t)
            if i == 0:
                for copy in weights(d):
                    copy.wait()
            lhs = jnp.concatenate([relaid[at(peer(2 * o + 1), h), :], relaid[at(peer(2 * o), h), :]], axis=0)
            for weight, w, start in ((psi_v, lz, 0), (ups_v, sz, lz)):
                both = jnp.dot(lhs, weight[:, block(d, w)], preferred_element_type=F32)
                xs[slot, d, :, start:start + w] = both[:half]
                keep[slot, d, :, start:start + w] = both[half:]
            swap_copy(i, d).start()

        def combine(t):
            d = chunk(t)
            swap_copy(i, d).wait_recv()
            total = keep[slot, d] + xr[i, d]

            @pl.when(t < first)
            def _():
                zs[i, d] = encode(total)
                near_copy(i, d).start()

            @pl.when(t >= first)
            def _():
                keep[slot, d] = total

        @pl.loop(0, m + LAG)
        def _(t):
            @pl.when(t < m)
            def _():
                product(t)

            @pl.when(t >= LAG)
            def _():
                combine(t - LAG)

    def relay(i):
        slot = i % slots

        @pl.loop(first, m - 1)
        def _(t):
            d = chunk(t)
            near_copy(i, d).wait_recv()
            zs[i, d] = encode(keep[slot, d] + decode(z1r[i, d]))
            far_copy(i, d).start()

    def give_back(i):
        o, h = pieces[i]
        near_copy(i, c).wait_recv()
        own_slot = own.at[h] if o == 0 else keep.at[i % slots, c]
        own_slot[...] = keep[i % slots, c] + decode(z1r[i, c])
        for g in range(m // 2):
            @pl.when(g != pair)
            def _():
                remote(zs.at[i, c], z2r.at[i, g], z_s, z2_s.at[i, g], {"col": near}).wait_recv()
                own_slot[...] += decode(z2r[i, g])
        if o:
            ys[i] = encode(own_slot[...])
            back_copy(i).start()

    def finish(h):
        received(yr.at[h, 1:], y_r.at[h])
        total = own[h]
        for o in range(1, chips):
            total = total + decode(yr[h, o])
        co_out[pl.ds(h * half, half), :] = total[:, :lz]
        gathered[at(me, h), :] = total[:, lz:].astype(BF16)
        for o in range(1, chips):
            spread_rows(o, h).start()
        pass_rows(0, h).start()

    tile = range_tile(width)
    tiles = width // tile

    def forward_omega():
        received(omega_all.at[:, pl.ds(0, (chips - 1) * depth)], g_r.at[2])
        for o in range(1, chips):
            pass_omega(o).start()

    def update_range():
        local[4].wait()
        received(omega_all.at[:, pl.ds(0, chips * depth)], f_r.at[2])

        @pl.loop(0, tiles)
        def _(j):
            range_v[:, block(j, tile)] += jnp.dot(omega_all[...], relaid[:, block(j, tile)], preferred_element_type=F32)

    def forward_rows(h):
        received(gathered.at[pl.ds(0, (chips - 1) * half), :], g_r.at[h])
        for o in range(1, chips):
            pass_rows(o, h).start()

    def wait_all():
        local[2].wait()
        local[5].wait()
        received(phi_all.at[:, pl.ds(0, (n - 1) * depth)], p_r)
        for h in range(2):
            received(gathered.at[pl.ds(0, chips * half), :], f_r.at[h])

    def update_core():
        core_out[...] += jnp.dot(phi_all[...], gathered[...], preferred_element_type=F32)

    count = len(pieces)

    def drain():
        sent(window.at[:, pl.ds(0, (n - 1) * width)], a_s)
        for i in range(count - slots, count):
            sent(xs.at[i % slots], x_s.at[i % slots])

    def drain_all():
        sent(zs.at[:, pl.ds(0, m - 1)], z_s)
        sent(ys.at[pl.ds(0, count - 2)], y_s)
        sent(phi.at[pl.ds(0, (n - 1) * core_rows), :], p_s)
        sent(omega_all.at[:, pl.ds(0, (chips - 1) * depth)], g_s.at[1])
        sent(omega_all.at[:, pl.ds(0, chips * depth)], f_s.at[1])
        sent(gathered.at[pl.ds(0, (chips - 1) * rows), :], g_s.at[0])
        sent(gathered.at[pl.ds(0, chips * rows), :], f_s.at[0])

    plan = []
    for step in range(count):
        plan += [(send_window, i) for i in range(count) if distant(i) and step == max(i - LEAD, 0)]
        if step == count - 2:
            plan.append((send_small,))
        plan.append((multiply, step))
        if step and step < count - 1:
            plan.append((relay, step - 1))
        if step >= 2:
            plan.append((give_back, step - 2))
        if step == count - 2:
            plan.append((relay, step))
    plan += [
        (give_back, count - 2), (relay, count - 1), (forward_omega,), (give_back, count - 1),
        (finish, 0), (finish, 1), (drain,), (update_range,), (forward_rows, 0), (forward_rows, 1), (wait_all,),
        (update_core,), (drain_all,)]
    for act, *which in plan:
        with mark("_".join([act.__name__, *map(str, which[:1])])):
            act(*which)


def store_kernel(*refs):
    *refs, sem = refs
    count = len(refs) // 2
    copies = [pltpu.make_async_copy(refs[i], refs[count + i], sem.at[i]) for i in range(count)]
    for copy in copies:
        copy.start()
    for copy in copies:
        copy.wait()


def range_tile(width):
    return min(width, 256)


def shards(n, m, window_rows, omega_cols, psi_rows, upsilon_rows, phi_cols, range_old, core_old):
    any_space = pl.BlockSpec(memory_space=pl.ANY)
    vmem = pl.BlockSpec(memory_space=pltpu.VMEM)
    dma = pltpu.SemaphoreType.DMA
    rows, wide = window_rows.shape
    width = wide // n
    k = omega_cols.shape[0]
    l, s = psi_rows.shape[1], upsilon_rows.shape[1]
    core_rows = phi_cols.shape[0] // n
    half, chips, cz = rows // 2, n // 2, (l + s) // m
    count = 2 * chips
    slots = min(count, 4)
    scratch = [
        pltpu.VMEM((rows * n, width), BF16), pltpu.VMEM((width, l), BF16), pltpu.VMEM((width, s), BF16),
        pltpu.VMEM((slots, m, half, cz), F32), pltpu.VMEM((count, m, half, cz), F32), pltpu.VMEM((slots, m, half, cz), F32),
        pltpu.VMEM((count, m, half, cz), BF16), pltpu.VMEM((count, m, half, cz), BF16), pltpu.VMEM((count, m // 2, half, cz), BF16),
        pltpu.VMEM((2, half, cz), F32), pltpu.VMEM((count, half, cz), BF16), pltpu.VMEM((2, chips, half, cz), BF16),
        pltpu.VMEM((rows * n, s // m), BF16), pltpu.VMEM((core_rows, rows * n), BF16), pltpu.VMEM((k, rows * n), BF16),
        dma((m, 2)), dma((6,)), dma, dma((n, 2)), dma, dma,
        dma((slots,)), dma((2, m)), dma, dma((count, m)), dma((count, m // 2)),
        dma, dma((2,)), dma((2,)), dma((3,)), dma((2,)), dma((3,)),
    ]
    outputs = (
        jax.ShapeDtypeStruct((k, width), F32), jax.ShapeDtypeStruct((rows, l // m), F32),
        jax.ShapeDtypeStruct((core_rows, s // m), F32))
    output_bytes = sum(4 * math.prod(out.shape) for out in outputs)
    results = pl.pallas_call(
        functools.partial(sketch_kernel, n, m),
        out_shape=outputs,
        in_specs=[any_space] * 7,
        out_specs=(vmem, vmem, vmem),
        scratch_shapes=scratch,
        compiler_params=pltpu.CompilerParams(collective_id=0, has_side_effects=True, vmem_limit_bytes=LIMIT - output_bytes - ROOM),
        name="sketch",
    )(*(pltpu.with_memory_space_constraint(x, pltpu.HBM) for x in (
        window_rows, omega_cols, psi_rows, upsilon_rows, phi_cols, range_old, core_old)))
    return pl.pallas_call(
        store_kernel,
        out_shape=outputs,
        in_specs=[vmem] * 3,
        out_specs=[any_space] * 3,
        scratch_shapes=[dma((3,))],
        compiler_params=pltpu.CompilerParams(vmem_limit_bytes=1024 * 1024),
        name="store",
    )(*results)


def solution(mesh):
    placed = (
        P("row", "col"),
        P(None, "row"),
        P(("col", "row"), None),
        P(("col", "row"), None),
        P(None, "row"),
        P(None, ("col", "row")),
        P("row", "col"),
    )
    return jax.shard_map(
        functools.partial(shards, mesh.shape["row"], mesh.shape["col"]),
        mesh=mesh,
        in_specs=placed,
        out_specs=(P(None, ("col", "row")), P("row", "col"), P("row", "col")),
        check_vma=False,
    )
```

```python
import contextlib
import functools
import math

import jax
import jax.numpy as jnp
from jax import lax
from jax.experimental import pallas as pl
from jax.experimental.pallas import tpu as pltpu
from jax.sharding import PartitionSpec as P

MESH = pl.DeviceIdType.MESH
LIMIT = 67043328
LEAD = 3
LAG = 2
ROOM = 13000 * 1024
F32, BF16 = jnp.float32, jnp.bfloat16


def mark(name):
    return contextlib.nullcontext()


def encode(x):
    return (x * jnp.abs(x)).astype(BF16)


def decode(y):
    y = y.astype(F32)
    return y * lax.rsqrt(jnp.maximum(jnp.abs(y), 1e-37))


def flip(index, mask, count):
    total, bit = 0, 1
    while bit < count:
        own = (index // bit) % 2
        total = total + (1 - own if mask & bit else own) * bit
        bit *= 2
    return total


def piece_order(chips):
    classes = {}
    for o in range(chips):
        classes.setdefault(bin(o).count("1"), []).append(o)
    return [(o, h) for k in sorted(classes) for h in range(2) for o in classes[k]]


def sketch_kernel(n, m, window, omega, psi, ups, phi, range_old, core_old, range_v, co_out, core_out,
                  relaid, psi_v, ups_v, xs, xr, keep, zs, z1r, z2r, own, ys, yr, gathered, phi_all, omega_all,
                  w_sem, l_sem, a_s, a_r, p_s, p_r, x_s, x_r, z_s, z1_s, z2_s, y_s, y_r, g_s, g_r, f_s, f_r):
    me, c = lax.axis_index("row"), lax.axis_index("col")
    chips = n // 2
    rows, width = window.shape[0], relaid.shape[1]
    half = rows // 2
    lz = psi_v.shape[1] // m
    sz = ups_v.shape[1] // m
    cz = lz + sz
    slots = keep.shape[0]
    core_rows, depth = phi_all.shape[0], phi.shape[1]
    dims = chips.bit_length() - 1
    pieces = piece_order(chips)
    odd = c % 2
    side = c + odd * (m - 1 - 2 * c)
    first = m - 1 - side
    near = c + 1 - 2 * odd
    pair = c // 2

    def at(r, h):
        return pl.ds(pl.multiple_of(r * rows + h * half, half), half)

    def block(r, size):
        return pl.ds(pl.multiple_of(r * size, size), size)

    def peer(mask):
        return flip(me, mask, n)

    def chunk(t):
        ahead = jnp.where(t < first, m - 1 - t, jnp.where(t < m - 1, t - first, side))
        return ahead + odd * (m - 1 - 2 * ahead)

    def remote(src, dst, send_sem, recv_sem, device):
        return pltpu.make_async_remote_copy(
            src_ref=src, dst_ref=dst, send_sem=send_sem, recv_sem=recv_sem, device_id=device, device_id_type=MESH)

    def sent(ref, sem):
        remote(ref, ref, sem, y_r.at[0], {"row": peer(1)}).wait_send()

    def received(ref, sem):
        remote(ref, ref, y_s, sem, {"row": peer(1)}).wait_recv()

    def weights(d):
        return (
            pltpu.make_async_copy(psi.at[:, block(d, lz)], psi_v.at[:, block(d, lz)], w_sem.at[d]),
            pltpu.make_async_copy(ups.at[:, block(d, sz)], ups_v.at[:, block(d, sz)], w_sem.at[d]))

    local = [
        pltpu.make_async_copy(window.at[pl.ds(h * half, half), block(me, width)], relaid.at[at(me, h), :], l_sem.at[h])
        for h in range(2)]
    local += [
        pltpu.make_async_copy(phi.at[block(me, core_rows), :], phi_all.at[:, block(me, depth)], l_sem.at[2]),
        pltpu.make_async_copy(omega, omega_all.at[:, block(me, depth)], l_sem.at[3]),
        pltpu.make_async_copy(range_old, range_v, l_sem.at[4]),
        pltpu.make_async_copy(core_old, core_out, l_sem.at[5])]

    def linked(d):
        low, high = jnp.minimum(c, d), jnp.maximum(c, d)
        return (d != c) & ((low // 2 == high // 2) | (high % 2 == 0) | (low % 2 == 1))

    barrier = pltpu.get_barrier_semaphore()
    greeted = n - 1
    for d in range(m):
        @pl.when(linked(d))
        def _():
            pl.semaphore_signal(barrier, inc=1, device_id={"col": d}, device_id_type=MESH)
        greeted = greeted + jnp.where(linked(d), 1, 0)
    for e in reversed(range(1, n)):
        pl.semaphore_signal(barrier, inc=1, device_id={"row": peer(e)}, device_id_type=MESH)
    for copy in local[:2]:
        copy.start()
    for t in range(m):
        for copy in weights(chunk(t)):
            copy.start()
    pl.semaphore_wait(barrier, greeted)

    def window_copy(e, h):
        return remote(window.at[pl.ds(h * half, half), block(peer(e), width)], relaid.at[at(me, h), :],
                      a_s, a_r.at[e // 2, h], {"row": peer(e)})

    def phi_copy(e):
        return remote(phi.at[block(peer(e), core_rows), :], phi_all.at[:, block(me, depth)],
                      p_s, p_r, {"row": peer(e)})

    def send_window(i):
        o, h = pieces[i]
        for e in (2 * o, 2 * o + 1):
            if e:
                window_copy(e, h).start()

    def distant_chip(o):
        return bin(o).count("1") > 1

    def distant(i):
        return distant_chip(pieces[i][0])

    for i in range(len(pieces)):
        if not distant(i):
            send_window(i)

    def omega_copy(o, g, j):
        rows_g = pl.ds(g * (omega.shape[0] // 2), omega.shape[0] // 2)
        place = omega_all.at[rows_g, block(peer(2 * o), depth)]
        source = place if o else omega.at[rows_g, :]
        return remote(source, place, g_s.at[1], g_r.at[2 + j], {"row": peer(2 << (j + g) % dims)})

    def omega_step(j):
        if j:
            received(omega_all.at[:, pl.ds(0, depth << (j - 1))], g_r.at[1 + j])
        for o in range(chips):
            for g in range(2):
                if all((o & 1 << (i + g) % dims) == 0 for i in range(j, dims)):
                    omega_copy(o, g, j).start()

    def pass_omega(o):
        place = omega_all.at[:, block(peer(2 * o), depth)]
        return remote(place, place, f_s.at[1], f_r.at[2], {"row": peer(1)})

    def spread_rows(o, h):
        place = gathered.at[at(me, h), :]
        return remote(place, place, g_s.at[0], g_r.at[h], {"row": peer(2 * o)})

    def pass_rows(o, h):
        place = gathered.at[at(peer(2 * o), h), :]
        return remote(place, place, f_s.at[0], f_r.at[h], {"row": peer(1)})

    for copy in local[2:]:
        copy.start()

    def send_small():
        omega_step(0)
        local[3].wait()
        pass_omega(0).start()

    def send_phi(part):
        for e in range(1, n):
            if (2 if distant_chip(e // 2) else e % 2) == part:
                phi_copy(e).start()

    def swap_copy(i, d):
        return remote(xs.at[i % slots, d], xr.at[i, d], x_s.at[i % slots], x_r.at[i % 2, d], {"row": peer(1)})

    def near_copy(i, d):
        return remote(zs.at[i, d], z1r.at[i, d], z_s, z1_s.at[i, d], {"col": near})

    def far_copy(i, d):
        return remote(zs.at[i, d], z2r.at[i, pair], z_s, z2_s.at[i], {"col": d})

    def back_copy(o, h):
        return remote(ys.at[h, o], yr.at[h, o], y_s, y_r.at[h], {"row": peer(2 * o)})

    def multiply(i):
        o, h = pieces[i]
        slot = i % slots
        if o == 0:
            local[h].wait()
            window_copy(1, h).wait_recv()
        else:
            received(relaid.at[pl.ds(0, 2 * half), :], a_r.at[o, h])
        if i >= slots:
            sent(xs.at[slot], x_s.at[slot])

        def product(t):
            d = chunk(t)
            if i == 0:
                both = ups_v.at[:, pl.ds(0, cz)]
                pltpu.make_async_copy(both, both, w_sem.at[d]).wait()
            lhs = jnp.concatenate([relaid[at(peer(2 * o + 1), h), :], relaid[at(peer(2 * o), h), :]], axis=0)
            for weight, w, start in ((psi_v, lz, 0), (ups_v, sz, lz)):
                both = jnp.dot(lhs, weight[:, block(d, w)], preferred_element_type=F32)
                xs[slot, d, :, start:start + w] = both[:half]
                keep[slot, d, :, start:start + w] = both[half:]
            swap_copy(i, d).start()

        def combine(t):
            d = chunk(t)
            swap_copy(i, d).wait_recv()
            total = keep[slot, d] + xr[i, d]

            @pl.when(t < first)
            def _():
                zs[i, d] = encode(total)
                near_copy(i, d).start()

            @pl.when(t >= first)
            def _():
                keep[slot, d] = total

        @pl.loop(0, m + LAG)
        def _(t):
            @pl.when(t < m)
            def _():
                product(t)

            @pl.when(t >= LAG)
            def _():
                combine(t - LAG)

    def relay(i):
        slot = i % slots

        @pl.loop(first, m - 1)
        def _(t):
            d = chunk(t)
            near_copy(i, d).wait_recv()
            zs[i, d] = encode(keep[slot, d] + decode(z1r[i, d]))
            far_copy(i, d).start()

    def give_back(i):
        o, h = pieces[i]
        near_copy(i, c).wait_recv()
        total = own.at[h, o]
        total[...] = keep[i % slots, c] + decode(z1r[i, c])
        if m > 2:
            received(z2r.at[i, pl.ds(0, m // 2 - 1)], z2_s.at[i])
        for g in range(m // 2):
            @pl.when(g != pair)
            def _():
                total[...] += decode(z2r[i, g])
        if o:
            ys[h, o] = encode(total[...])
            back_copy(o, h).start()

    def finish(h):
        received(yr.at[h, pl.ds(1, chips - 1)], y_r.at[h])
        total = own[h, 0]
        for o in range(1, chips):
            total = total + decode(yr[h, o])
        co_out[pl.ds(h * half, half), :] = total[:, :lz]
        gathered[at(me, h), :] = total[:, lz:].astype(BF16)
        for o in range(1, chips):
            spread_rows(o, h).start()
        pass_rows(0, h).start()

    tile = range_tile(width)
    tiles = width // tile

    def forward_omega():
        received(omega_all.at[:, pl.ds(0, depth << (dims - 1))], g_r.at[1 + dims])
        for o in range(1, chips):
            pass_omega(o).start()

    def update_range():
        local[4].wait()
        received(omega_all.at[:, pl.ds(0, chips * depth)], f_r.at[2])

        @pl.loop(0, tiles)
        def _(j):
            range_v[:, block(j, tile)] += jnp.dot(omega_all[...], relaid[:, block(j, tile)], preferred_element_type=F32)

    def forward_rows(h):
        received(gathered.at[pl.ds(0, (chips - 1) * half), :], g_r.at[h])
        for o in range(1, chips):
            pass_rows(o, h).start()

    def wait_all():
        local[2].wait()
        local[5].wait()
        received(phi_all.at[:, pl.ds(0, (n - 1) * depth)], p_r)
        for h in range(2):
            received(gathered.at[pl.ds(0, chips * half), :], f_r.at[h])

    def update_core():
        core_out[...] += jnp.dot(phi_all[...], gathered[...], preferred_element_type=F32)

    count = len(pieces)

    def drain():
        sent(window.at[:, pl.ds(0, (n - 1) * width)], a_s)
        for i in range(count - slots, count):
            sent(xs.at[i % slots], x_s.at[i % slots])

    def drain_all():
        sent(zs.at[:, pl.ds(0, m - 1)], z_s)
        sent(ys.at[:, pl.ds(1, chips - 1)], y_s)
        sent(phi.at[pl.ds(0, (n - 1) * core_rows), :], p_s)
        sent(omega_all.at[:, pl.ds(0, (chips - 1) * depth)], g_s.at[1])
        sent(omega_all.at[:, pl.ds(0, chips * depth)], f_s.at[1])
        sent(gathered.at[pl.ds(0, (chips - 1) * rows), :], g_s.at[0])
        sent(gathered.at[pl.ds(0, chips * rows), :], f_s.at[0])

    plan = []
    for step in range(count):
        plan += [(send_window, i) for i in range(count) if distant(i) and step == max(i - LEAD, 0)]
        if step == count - 2:
            plan.append((send_small,))
            plan += [(send_phi, p) for p in range(3)]
        plan.append((multiply, step))
        if step and step < count - 1:
            plan.append((relay, step - 1))
        if step >= 2:
            plan.append((give_back, step - 2))
        if step == count - 2:
            plan.append((relay, step))
    plan += [(give_back, count - 2)]
    plan += [(omega_step, j) for j in range(1, dims)]
    plan += [
        (relay, count - 1), (give_back, count - 1), (forward_omega,), (finish, 0), (finish, 1), (drain,), (update_range,),
        (forward_rows, 0), (forward_rows, 1), (wait_all,), (update_core,), (drain_all,)]
    for act, *which in plan:
        with mark("_".join([act.__name__, *map(str, which[:1])])):
            act(*which)


def store_kernel(*refs):
    *refs, sem = refs
    count = len(refs) // 2
    copies = [pltpu.make_async_copy(refs[i], refs[count + i], sem.at[i]) for i in range(count)]
    for copy in copies:
        copy.start()
    for copy in copies:
        copy.wait()


def range_tile(width):
    return min(width, 256)


def shards(n, m, window_rows, omega_cols, psi_rows, upsilon_rows, phi_cols, range_old, core_old):
    any_space = pl.BlockSpec(memory_space=pl.ANY)
    vmem = pl.BlockSpec(memory_space=pltpu.VMEM)
    dma = pltpu.SemaphoreType.DMA
    rows, wide = window_rows.shape
    width = wide // n
    k = omega_cols.shape[0]
    l, s = psi_rows.shape[1], upsilon_rows.shape[1]
    core_rows = phi_cols.shape[0] // n
    half, chips, cz = rows // 2, n // 2, (l + s) // m
    count = 2 * chips
    slots = min(count, 4)
    scratch = [
        pltpu.VMEM((rows * n, width), BF16), pltpu.VMEM((width, l), BF16), pltpu.VMEM((width, s), BF16),
        pltpu.VMEM((slots, m, half, cz), F32), pltpu.VMEM((count, m, half, cz), F32), pltpu.VMEM((slots, m, half, cz), F32),
        pltpu.VMEM((count, m, half, cz), BF16), pltpu.VMEM((count, m, half, cz), BF16), pltpu.VMEM((count, m // 2, half, cz), BF16),
        pltpu.VMEM((2, chips, half, cz), F32), pltpu.VMEM((2, chips, half, cz), BF16), pltpu.VMEM((2, chips, half, cz), BF16),
        pltpu.VMEM((rows * n, s // m), BF16), pltpu.VMEM((core_rows, rows * n), BF16), pltpu.VMEM((k, rows * n), BF16),
        dma((m,)), dma((6,)), dma, dma((chips, 2)), dma, dma,
        dma((slots,)), dma((2, m)), dma, dma((count, m)), dma((count,)),
        dma, dma((2,)), dma((2,)), dma((2 + chips.bit_length() - 1,)), dma((2,)), dma((3,)),
    ]
    outputs = (
        jax.ShapeDtypeStruct((k, width), F32), jax.ShapeDtypeStruct((rows, l // m), F32),
        jax.ShapeDtypeStruct((core_rows, s // m), F32))
    output_bytes = sum(4 * math.prod(out.shape) for out in outputs)
    results = pl.pallas_call(
        functools.partial(sketch_kernel, n, m),
        out_shape=outputs,
        in_specs=[any_space] * 7,
        out_specs=(vmem, vmem, vmem),
        scratch_shapes=scratch,
        compiler_params=pltpu.CompilerParams(collective_id=0, has_side_effects=True, vmem_limit_bytes=LIMIT - output_bytes - ROOM),
        name="sketch",
    )(*(pltpu.with_memory_space_constraint(x, pltpu.HBM) for x in (
        window_rows, omega_cols, psi_rows, upsilon_rows, phi_cols, range_old, core_old)))
    return pl.pallas_call(
        store_kernel,
        out_shape=outputs,
        in_specs=[vmem] * 3,
        out_specs=[any_space] * 3,
        scratch_shapes=[dma((3,))],
        compiler_params=pltpu.CompilerParams(vmem_limit_bytes=1024 * 1024),
        name="store",
    )(*results)


def solution(mesh):
    placed = (
        P("row", "col"),
        P(None, "row"),
        P(("col", "row"), None),
        P(("col", "row"), None),
        P(None, "row"),
        P(None, ("col", "row")),
        P("row", "col"),
    )
    return jax.shard_map(
        functools.partial(shards, mesh.shape["row"], mesh.shape["col"]),
        mesh=mesh,
        in_specs=placed,
        out_specs=(P(None, ("col", "row")), P("row", "col"), P("row", "col")),
        check_vma=False,
    )
```

```python
import contextlib
import functools
import math

import jax
import jax.numpy as jnp
from jax import lax
from jax.experimental import pallas as pl
from jax.experimental.pallas import tpu as pltpu
from jax.sharding import PartitionSpec as P

MESH = pl.DeviceIdType.MESH
LIMIT = 67043328
LEAD = 3
LAG = 2
ROOM = 13000 * 1024
F32, BF16 = jnp.float32, jnp.bfloat16


def mark(name):
    return contextlib.nullcontext()


def encode(x):
    return (x * jnp.abs(x)).astype(BF16)


def decode(y):
    y = y.astype(F32)
    return y * lax.rsqrt(jnp.maximum(jnp.abs(y), 1e-37))


def flip(index, mask, count):
    total, bit = 0, 1
    while bit < count:
        own = (index // bit) % 2
        total = total + (1 - own if mask & bit else own) * bit
        bit *= 2
    return total


def piece_order(chips):
    classes = {}
    for o in range(chips):
        classes.setdefault(bin(o).count("1"), []).append(o)
    return [(o, h) for k in sorted(classes) for h in range(2) for o in classes[k]]


def sketch_kernel(n, m, window, omega, psi, ups, phi, range_old, core_old, range_v, co_out, core_out,
                  relaid, psi_v, ups_v, xs, xr, keep, zs, z1r, z2r, own, ys, yr, gathered, phi_all, omega_all,
                  w_sem, l_sem, a_s, a_r, p_s, p_r, x_s, x_r, z_s, z1_s, z2_s, y_s, y_r, g_s, g_r, f_s, f_r, q_s, q_r):
    me, c = lax.axis_index("row"), lax.axis_index("col")
    chips = n // 2
    rows, width = window.shape[0], relaid.shape[1]
    half = rows // 2
    lz = psi_v.shape[1] // m
    sz = ups_v.shape[1] // m
    cz = lz + sz
    slots = keep.shape[0]
    core_rows, depth = phi_all.shape[0], phi.shape[1]
    dims = chips.bit_length() - 1
    pieces = piece_order(chips)
    odd = c % 2
    side = c + odd * (m - 1 - 2 * c)
    first = m - 1 - side
    near = c + 1 - 2 * odd
    pair = c // 2

    def at(r, h):
        return pl.ds(pl.multiple_of(r * rows + h * half, half), half)

    def block(r, size):
        return pl.ds(pl.multiple_of(r * size, size), size)

    def peer(mask):
        return flip(me, mask, n)

    def chunk(t):
        ahead = jnp.where(t < first, m - 1 - t, jnp.where(t < m - 1, t - first, side))
        return ahead + odd * (m - 1 - 2 * ahead)

    def remote(src, dst, send_sem, recv_sem, device):
        return pltpu.make_async_remote_copy(
            src_ref=src, dst_ref=dst, send_sem=send_sem, recv_sem=recv_sem, device_id=device, device_id_type=MESH)

    def sent(ref, sem):
        remote(ref, ref, sem, y_r.at[0], {"row": peer(1)}).wait_send()

    def received(ref, sem):
        remote(ref, ref, y_s, sem, {"row": peer(1)}).wait_recv()

    share = core_rows // m

    def phi_rows(r):
        return pl.ds(pl.multiple_of(r * core_rows + c * share, share), share)

    def weights(d):
        return (
            pltpu.make_async_copy(psi.at[:, block(d, lz)], psi_v.at[:, block(d, lz)], w_sem.at[d]),
            pltpu.make_async_copy(ups.at[:, block(d, sz)], ups_v.at[:, block(d, sz)], w_sem.at[d]))

    local = [
        pltpu.make_async_copy(window.at[pl.ds(h * half, half), block(me, width)], relaid.at[at(me, h), :], l_sem.at[h])
        for h in range(2)]
    local += [
        pltpu.make_async_copy(phi.at[phi_rows(me), :], phi_all.at[block(c, share), block(me, depth)], l_sem.at[2]),
        pltpu.make_async_copy(omega, omega_all.at[:, block(me, depth)], l_sem.at[3]),
        pltpu.make_async_copy(range_old, range_v, l_sem.at[4]),
        pltpu.make_async_copy(core_old, core_out, l_sem.at[5])]

    def linked(d):
        low, high = jnp.minimum(c, d), jnp.maximum(c, d)
        return (d != c) & ((low // 2 == high // 2) | (high % 2 == 0) | (low % 2 == 1))

    barrier = pltpu.get_barrier_semaphore()
    greeted = n - 1
    for d in range(m):
        @pl.when(linked(d))
        def _():
            pl.semaphore_signal(barrier, inc=1, device_id={"col": d}, device_id_type=MESH)
        greeted = greeted + jnp.where(linked(d), 1, 0)
    for e in reversed(range(1, n)):
        pl.semaphore_signal(barrier, inc=1, device_id={"row": peer(e)}, device_id_type=MESH)
    for copy in local[:2]:
        copy.start()
    for t in range(m):
        for copy in weights(chunk(t)):
            copy.start()
    pl.semaphore_wait(barrier, greeted)

    def window_copy(e, h):
        return remote(window.at[pl.ds(h * half, half), block(peer(e), width)], relaid.at[at(me, h), :],
                      a_s, a_r.at[e // 2, h], {"row": peer(e)})

    def phi_copy(e):
        return remote(phi.at[phi_rows(peer(e)), :], phi_all.at[block(c, share), block(me, depth)], p_s, p_r, {"row": peer(e)})

    def ring_copy(way, step):
        quarter = phi_all.at[block(c - way * (step - 1), share), :]
        return remote(quarter, quarter, q_s.at[(way + 1) // 2, step - 1], q_r.at[(way + 1) // 2, step - 1], {"col": c + way})

    def ring_sends(way, step):
        source, target = c - way * (step - 1), c + way
        return (source >= 0) & (source < m) & (target >= 0) & (target < m)

    def ring_gets(way, step):
        source = c - way * step
        return (source >= 0) & (source < m)

    def ring_wait(step):
        for way in (-1, 1):
            @pl.when(ring_gets(way, step))
            def _():
                received(phi_all.at[pl.ds(0, share), :], q_r.at[(way + 1) // 2, step - 1])

    def ring_phi(step):
        if step == 1:
            local[2].wait()
            received(phi_all.at[pl.ds(0, share), pl.ds(0, (n - 1) * depth)], p_r)
        else:
            ring_wait(step - 1)
        for way in (-1, 1):
            @pl.when(ring_sends(way, step))
            def _():
                ring_copy(way, step).start()

    def send_window(i):
        o, h = pieces[i]
        for e in (2 * o, 2 * o + 1):
            if e:
                window_copy(e, h).start()

    def distant_chip(o):
        return bin(o).count("1") > 1

    def distant(i):
        return distant_chip(pieces[i][0])

    for i in range(len(pieces)):
        if not distant(i):
            send_window(i)

    def omega_copy(o, g, j):
        rows_g = pl.ds(g * (omega.shape[0] // 2), omega.shape[0] // 2)
        place = omega_all.at[rows_g, block(peer(2 * o), depth)]
        source = place if o else omega.at[rows_g, :]
        return remote(source, place, g_s.at[1], g_r.at[2 + j], {"row": peer(2 << (j + g) % dims)})

    def omega_step(j):
        if j:
            received(omega_all.at[:, pl.ds(0, depth << (j - 1))], g_r.at[1 + j])
        for o in range(chips):
            for g in range(2):
                if all((o & 1 << (i + g) % dims) == 0 for i in range(j, dims)):
                    omega_copy(o, g, j).start()

    def pass_omega(o):
        place = omega_all.at[:, block(peer(2 * o), depth)]
        return remote(place, place, f_s.at[1], f_r.at[2], {"row": peer(1)})

    def spread_rows(o, h):
        place = gathered.at[at(me, h), :]
        return remote(place, place, g_s.at[0], g_r.at[h], {"row": peer(2 * o)})

    def pass_rows(o, h):
        place = gathered.at[at(peer(2 * o), h), :]
        return remote(place, place, f_s.at[0], f_r.at[h], {"row": peer(1)})

    for copy in local[2:]:
        copy.start()

    def send_small():
        omega_step(0)
        local[3].wait()
        pass_omega(0).start()

    def send_phi():
        for e in range(1, n):
            phi_copy(e).start()

    def swap_copy(i, d):
        return remote(xs.at[i % slots, d], xr.at[i, d], x_s.at[i % slots], x_r.at[i % 2, d], {"row": peer(1)})

    def near_copy(i, d):
        return remote(zs.at[i, d], z1r.at[i, d], z_s, z1_s.at[i, d], {"col": near})

    def far_copy(i, d):
        return remote(zs.at[i, d], z2r.at[i, pair], z_s, z2_s.at[i], {"col": d})

    def back_copy(o, h):
        return remote(ys.at[h, o], yr.at[h, o], y_s, y_r.at[h], {"row": peer(2 * o)})

    def multiply(i):
        o, h = pieces[i]
        slot = i % slots
        if o == 0:
            local[h].wait()
            window_copy(1, h).wait_recv()
        else:
            received(relaid.at[pl.ds(0, 2 * half), :], a_r.at[o, h])
        if i >= slots:
            sent(xs.at[slot], x_s.at[slot])

        def product(t):
            d = chunk(t)
            if i == 0:
                both = ups_v.at[:, pl.ds(0, cz)]
                pltpu.make_async_copy(both, both, w_sem.at[d]).wait()
            lhs = jnp.concatenate([relaid[at(peer(2 * o + 1), h), :], relaid[at(peer(2 * o), h), :]], axis=0)
            for weight, w, start in ((psi_v, lz, 0), (ups_v, sz, lz)):
                both = jnp.dot(lhs, weight[:, block(d, w)], preferred_element_type=F32)
                xs[slot, d, :, start:start + w] = both[:half]
                keep[slot, d, :, start:start + w] = both[half:]
            swap_copy(i, d).start()

        def combine(t):
            d = chunk(t)
            swap_copy(i, d).wait_recv()
            total = keep[slot, d] + xr[i, d]

            @pl.when(t < first)
            def _():
                zs[i, d] = encode(total)
                near_copy(i, d).start()

            @pl.when(t >= first)
            def _():
                keep[slot, d] = total

        @pl.loop(0, m + LAG)
        def _(t):
            @pl.when(t < m)
            def _():
                product(t)

            @pl.when(t >= LAG)
            def _():
                combine(t - LAG)

    def relay(i):
        slot = i % slots

        @pl.loop(first, m - 1)
        def _(t):
            d = chunk(t)
            near_copy(i, d).wait_recv()
            zs[i, d] = encode(keep[slot, d] + decode(z1r[i, d]))
            far_copy(i, d).start()

    def give_back(i):
        o, h = pieces[i]
        near_copy(i, c).wait_recv()
        total = own.at[h, o]
        total[...] = keep[i % slots, c] + decode(z1r[i, c])
        if m > 2:
            received(z2r.at[i, pl.ds(0, m // 2 - 1)], z2_s.at[i])
        for g in range(m // 2):
            @pl.when(g != pair)
            def _():
                total[...] += decode(z2r[i, g])
        if o:
            ys[h, o] = encode(total[...])
            back_copy(o, h).start()

    def finish(h):
        received(yr.at[h, pl.ds(1, chips - 1)], y_r.at[h])
        total = own[h, 0]
        for o in range(1, chips):
            total = total + decode(yr[h, o])
        co_out[pl.ds(h * half, half), :] = total[:, :lz]
        gathered[at(me, h), :] = total[:, lz:].astype(BF16)
        for o in range(1, chips):
            spread_rows(o, h).start()
        pass_rows(0, h).start()

    tile = range_tile(width)
    tiles = width // tile

    def forward_omega():
        received(omega_all.at[:, pl.ds(0, depth << (dims - 1))], g_r.at[1 + dims])
        for o in range(1, chips):
            pass_omega(o).start()

    def update_range():
        local[4].wait()
        received(omega_all.at[:, pl.ds(0, chips * depth)], f_r.at[2])

        @pl.loop(0, tiles)
        def _(j):
            range_v[:, block(j, tile)] += jnp.dot(omega_all[...], relaid[:, block(j, tile)], preferred_element_type=F32)

    def forward_rows(h):
        received(gathered.at[pl.ds(0, (chips - 1) * half), :], g_r.at[h])
        for o in range(1, chips):
            pass_rows(o, h).start()

    def wait_all():
        local[5].wait()
        ring_wait(m - 1)
        for h in range(2):
            received(gathered.at[pl.ds(0, chips * half), :], f_r.at[h])

    def update_core():
        core_out[...] += jnp.dot(phi_all[...], gathered[...], preferred_element_type=F32)

    count = len(pieces)

    def drain():
        sent(window.at[:, pl.ds(0, (n - 1) * width)], a_s)
        for i in range(count - slots, count):
            sent(xs.at[i % slots], x_s.at[i % slots])

    def drain_all():
        sent(zs.at[:, pl.ds(0, m - 1)], z_s)
        sent(ys.at[:, pl.ds(1, chips - 1)], y_s)
        sent(phi.at[pl.ds(0, (n - 1) * share), :], p_s)
        for step in range(1, m):
            for way in (-1, 1):
                @pl.when(ring_sends(way, step))
                def _():
                    sent(phi_all.at[pl.ds(0, share), :], q_s.at[(way + 1) // 2, step - 1])

        sent(omega_all.at[:, pl.ds(0, (chips - 1) * depth)], g_s.at[1])
        sent(omega_all.at[:, pl.ds(0, chips * depth)], f_s.at[1])
        sent(gathered.at[pl.ds(0, (chips - 1) * rows), :], g_s.at[0])
        sent(gathered.at[pl.ds(0, chips * rows), :], f_s.at[0])

    plan = []
    for step in range(count):
        plan += [(send_window, i) for i in range(count) if distant(i) and step == max(i - LEAD, 0)]
        if step == count - 2:
            plan += [(send_phi,), (send_small,)]
        plan.append((multiply, step))
        if step and step < count - 1:
            plan.append((relay, step - 1))
        if step >= 2:
            plan.append((give_back, step - 2))
        if step == count - 2:
            plan.append((relay, step))
    plan += [(give_back, count - 2)]
    plan += [(omega_step, j) for j in range(1, dims)]
    plan += [
        (relay, count - 1), (ring_phi, 1), (give_back, count - 1), (ring_phi, 2), (forward_omega,), (finish, 0), (finish, 1),
        *((ring_phi, step) for step in range(3, m)), (drain,), (update_range,),
        (forward_rows, 0), (forward_rows, 1), (wait_all,), (update_core,), (drain_all,)]
    for act, *which in plan:
        with mark("_".join([act.__name__, *map(str, which[:1])])):
            act(*which)


def store_kernel(*refs):
    *refs, sem = refs
    count = len(refs) // 2
    copies = [pltpu.make_async_copy(refs[i], refs[count + i], sem.at[i]) for i in range(count)]
    for copy in copies:
        copy.start()
    for copy in copies:
        copy.wait()


def range_tile(width):
    return min(width, 256)


def shards(n, m, window_rows, omega_cols, psi_rows, upsilon_rows, phi_cols, range_old, core_old):
    any_space = pl.BlockSpec(memory_space=pl.ANY)
    vmem = pl.BlockSpec(memory_space=pltpu.VMEM)
    dma = pltpu.SemaphoreType.DMA
    rows, wide = window_rows.shape
    width = wide // n
    k = omega_cols.shape[0]
    l, s = psi_rows.shape[1], upsilon_rows.shape[1]
    core_rows = phi_cols.shape[0] // n
    half, chips, cz = rows // 2, n // 2, (l + s) // m
    count = 2 * chips
    slots = min(count, 4)
    scratch = [
        pltpu.VMEM((rows * n, width), BF16), pltpu.VMEM((width, l), BF16), pltpu.VMEM((width, s), BF16),
        pltpu.VMEM((slots, m, half, cz), F32), pltpu.VMEM((count, m, half, cz), F32), pltpu.VMEM((slots, m, half, cz), F32),
        pltpu.VMEM((count, m, half, cz), BF16), pltpu.VMEM((count, m, half, cz), BF16), pltpu.VMEM((count, m // 2, half, cz), BF16),
        pltpu.VMEM((2, chips, half, cz), F32), pltpu.VMEM((2, chips, half, cz), BF16), pltpu.VMEM((2, chips, half, cz), BF16),
        pltpu.VMEM((rows * n, s // m), BF16), pltpu.VMEM((core_rows, rows * n), BF16), pltpu.VMEM((k, rows * n), BF16),
        dma((m,)), dma((6,)), dma, dma((chips, 2)), dma, dma,
        dma((slots,)), dma((2, m)), dma, dma((count, m)), dma((count,)),
        dma, dma((2,)), dma((2,)), dma((2 + chips.bit_length() - 1,)), dma((2,)), dma((3,)), dma((2, m - 1)), dma((2, m - 1)),
    ]
    outputs = (
        jax.ShapeDtypeStruct((k, width), F32), jax.ShapeDtypeStruct((rows, l // m), F32),
        jax.ShapeDtypeStruct((core_rows, s // m), F32))
    output_bytes = sum(4 * math.prod(out.shape) for out in outputs)
    results = pl.pallas_call(
        functools.partial(sketch_kernel, n, m),
        out_shape=outputs,
        in_specs=[any_space] * 7,
        out_specs=(vmem, vmem, vmem),
        scratch_shapes=scratch,
        compiler_params=pltpu.CompilerParams(collective_id=0, has_side_effects=True, vmem_limit_bytes=LIMIT - output_bytes - ROOM),
        name="sketch",
    )(*(pltpu.with_memory_space_constraint(x, pltpu.HBM) for x in (
        window_rows, omega_cols, psi_rows, upsilon_rows, phi_cols, range_old, core_old)))
    return pl.pallas_call(
        store_kernel,
        out_shape=outputs,
        in_specs=[vmem] * 3,
        out_specs=[any_space] * 3,
        scratch_shapes=[dma((3,))],
        compiler_params=pltpu.CompilerParams(vmem_limit_bytes=1024 * 1024),
        name="store",
    )(*results)


def solution(mesh):
    placed = (
        P("row", "col"),
        P(None, "row"),
        P(("col", "row"), None),
        P(("col", "row"), None),
        P(None, "row"),
        P(None, ("col", "row")),
        P("row", "col"),
    )
    return jax.shard_map(
        functools.partial(shards, mesh.shape["row"], mesh.shape["col"]),
        mesh=mesh,
        in_specs=placed,
        out_specs=(P(None, ("col", "row")), P("row", "col"), P("row", "col")),
        check_vma=False,
    )
```
